32 devices in a mesh: dp: 8 (over z, y), tr: 2 (over core), tc: 2 (over x).
Axes of the slice: x: 2, y: 2, z: 4, core: 2. Of those that a mesh axis runs over, the one named last changes fastest.
Arguments:
- activations: bfloat16 [4096, 4096], P('dp', ('tr', 'tc')), may hold values from -16.8 to 16.8, as said below
- gradients: bfloat16 [4096, 7168], P('dp', ('tr', 'tc')), may hold values from -16.8 to 16.8, as said below
- old_inputs: float32 [4096, 4096], P(('dp', 'tr', 'tc')), may hold values from -3 to 3
- old_gradients: float32 [7168, 7168], P(('dp', 'tr', 'tc')), may hold values from -3 to 3
Outputs:
- input_factor: float32 [4096, 4096], P(('dp', 'tr', 'tc'))
- grad_factor: float32 [7168, 7168], P(('dp', 'tr', 'tc'))
The draws below stay inside these ranges and needn't reach their ends.
Inputs may be any that keep to these rules, and one draw needn't show every extreme that they name: `activations`: real-valued samples. `gradients`: real-valued samples.
All inputs are finite; a program needn't handle non-finite values.
Results may differ from the reference program's by a relative error of at most 0.0045.
Values may be sent and summed in bfloat16 or wider, within the bound.
A program may use at most 192 MiB of HBM per device.

```python
import jax
import jax.numpy as jnp
from jax import lax

D = 4096
FF = 7168
TOK_DEV = 512
N_DP = 8


def spiked(key, width):
    first = jax.random.fold_in(key, 0)
    third = jax.random.fold_in(key, 2)
    rows_total = TOK_DEV * N_DP
    base = jnp.clip(jax.random.normal(first, (rows_total, width), jnp.float32), -6.0, 6.0)
    pairing = jax.random.permutation(third, N_DP).astype(jnp.int32)
    replica = jnp.arange(rows_total, dtype=jnp.int32) // TOK_DEV
    block = jnp.arange(width, dtype=jnp.int32) // (width // N_DP)
    target = jnp.take(pairing, replica)
    boost = jnp.where(target[:, None] == block[None, :], 2.0, 1.0)
    return (base * boost).astype(jnp.bfloat16)


def draw_activations(key, part):
    return spiked(jax.random.fold_in(key, 11), D)


def draw_gradients(key, part):
    return spiked(jax.random.fold_in(key, 23), FF)


def levels(key, dims, cuts, low, largest):
    factor_of, own = 1.0, jax.random.fold_in(key, 6)
    for axis_at, blocks in cuts:
        heights = jnp.exp(jax.random.uniform(jax.random.fold_in(own, axis_at), (blocks,), jnp.float32, low / len(cuts), largest / len(cuts)))
        factor_of = factor_of * jnp.repeat(heights, dims[axis_at] // blocks).reshape([-1 if axis == axis_at else 1 for axis in range(len(dims))])
    return factor_of


def bell_draw(own_key, shape, scale, most, cuts=(), kind=jnp.bfloat16):
    entries = scale * jax.random.normal(own_key, shape, jnp.float32)
    if cuts:
        entries = entries * levels(own_key, shape, cuts, -0.22, 0.18)
    return jnp.clip(entries, -most, most).astype(kind)


def setup_inputs(seed: int = 0) -> dict:
    key_list = jax.random.split(jax.random.key(seed), 5)
    activations = draw_activations(jax.random.fold_in(key_list[4], 71), 0)
    gradients = draw_gradients(jax.random.fold_in(key_list[4], 71), 0)
    old_inputs = bell_draw(key_list[2], (D, D), 0.5, 3.0, ((0, 32),), jnp.float32)
    old_gradients = bell_draw(key_list[3], (FF, FF), 0.5, 3.0, ((0, 32),), jnp.float32)
    return {"activations": activations, "gradients": gradients, "old_inputs": old_inputs, "old_gradients": old_gradients}


def replica_sum(samples, tokens_all):
    columns = samples.shape[1]
    replicas = samples.reshape(N_DP, TOK_DEV, columns)

    def accumulate(running, replica_rows):
        partial_value = (jnp.dot(replica_rows.T, replica_rows, preferred_element_type=jnp.float32) / tokens_all).astype(jnp.bfloat16)
        return running + partial_value.astype(jnp.float32), None

    running, _ = lax.scan(accumulate, jnp.zeros((columns, columns), jnp.float32), replicas)
    return running


def reference(activations, gradients, old_inputs, old_gradients):
    tokens_all = N_DP * TOK_DEV
    input_new = replica_sum(activations, tokens_all)
    gradient_new = replica_sum(gradients, tokens_all)
    return (0.5 * old_inputs + 0.5 * input_new, 0.5 * old_gradients + 0.5 * gradient_new)
```

```python
import jax
import jax.numpy as jnp
from jax import lax
from jax.sharding import Mesh, PartitionSpec as P

CELL = ("near", "tr", "tc")


def split_mesh(mesh):
    far, near = mesh.shape["dp"] // 2, 2
    rest = tuple(mesh.shape[name] for name in mesh.axis_names[1:])
    devices = mesh.devices.reshape((far, near) + rest)
    return Mesh(devices, ("far", "near") + tuple(mesh.axis_names[1:]))


def swap(block, name):
    return lax.ppermute(block, name, [(0, 1), (1, 0)])


def gather_pieces(samples):
    half = samples.shape[0] // 2
    over_near = swap(samples, "near")
    over_tc = swap(samples, "tc")
    first = swap(over_tc[:half], "near")
    second = swap(over_near[half:], "tc")
    pieces = ((samples, over_near), (over_tc, first, second))
    other = tuple(tuple(swap(block, "tr") for block in piece) for piece in pieces)
    return pieces, other


def assemble(pieces, other):
    tr, tc = lax.axis_index("tr"), lax.axis_index("tc")
    columns = pieces[0][0].shape[1]
    tokens = 2 * pieces[0][0].shape[0]
    wide = jnp.zeros((tokens, 4 * columns), pieces[0][0].dtype)
    for flip_tr, group in ((0, pieces), (1, other)):
        for flip_tc, piece in ((0, group[0]), (1, group[1])):
            at = ((tr ^ flip_tr) * 2 + (tc ^ flip_tc)) * columns
            row = 0
            for block in piece:
                wide = lax.dynamic_update_slice(wide, block, (row, at))
                row += block.shape[0]
    return wide


def partial_terms(wide, width, scale):
    cells = lax.axis_size(CELL)
    cell = lax.axis_index(CELL)
    tokens, features = wide.shape
    blocks = wide.reshape(tokens, features // (cells * width), cells, width)
    left = lax.dynamic_index_in_dim(blocks, cell, 2, keepdims=False)
    left = left.reshape(tokens, -1)
    product = lax.dot_general(
        left, wide, (((0,), (0,)), ((), ())), preferred_element_type=jnp.float32
    )
    return (product * scale).astype(jnp.bfloat16)


def body(activations, gradients, old_inputs, old_gradients):
    scale = 1.0 / (activations.shape[0] * lax.axis_size(("far", "near")))
    act_pieces = gather_pieces(activations)
    gradients, act_pieces = lax.optimization_barrier((gradients, act_pieces))
    grad_pieces = gather_pieces(gradients)
    outs = []
    for pieces, old in ((act_pieces, old_inputs), (grad_pieces, old_gradients)):
        part = partial_terms(assemble(*pieces), old.shape[0], scale)
        new = lax.psum_scatter(part, "far", scatter_dimension=0, tiled=True)
        outs.append(0.5 * old + 0.5 * new.astype(jnp.float32))
    return tuple(outs)


def solution(mesh):
    rows = ("far", "near", "tr", "tc")
    return jax.shard_map(
        body,
        mesh=split_mesh(mesh),
        in_specs=(
            P(("far", "near"), ("tr", "tc")),
            P(("far", "near"), ("tr", "tc")),
            P(rows, None),
            P(rows, None),
        ),
        out_specs=(P(rows, None), P(rows, None)),
        check_vma=False,
    )
```
